256 devices in a mesh: src: 64 (over x, z, core), grp: 4 (over y).
Axes of the slice: x: 4, y: 4, z: 8, core: 2. Of those that a mesh axis runs over, the one named last changes fastest.
Arguments:
- currents: bfloat16 [524288, 1024], P(('src', 'grp')), may hold values from -6 to 6
- leaf_basis: bfloat16 [2, 40, 524288], P(None, None, ('src', 'grp')), may hold values from -6 to 6
- leaf_box: int32 [524288], P(('src', 'grp')), may hold values from 0 to 7, as said below
- box_count: int32 [2048], P(('src', 'grp')), may hold values from 1 to 2041, as said below
- merge_factor: bfloat16 [2, 2560, 81920], P(None, None, ('src', 'grp')), may hold values from -0.25 to 0.25
- angle_factor: bfloat16 [4096, 4, 2, 2560], P('src'), may hold values from -0.0390625 to 0.0390625
Outputs:
- normalized: float32 [4096, 512], P('src', 'grp')
- peak_value: float32 [512], P('grp')
The draws below stay inside these ranges and needn't reach their ends.
Inputs may be any that keep to these rules, and one draw needn't show every extreme that they name: `leaf_box`: every source block of 2048 currents holds one or more currents of each of its 8 leaf boxes; some blocks put all but 7 of their currents into one box. box_count[k * 8 + b] is the number of currents of source block k whose leaf_box is b.
All inputs are finite; a program needn't handle non-finite values.
Results may differ from the reference program's by a relative error of at most 0.0057.
Values may be sent and summed in bfloat16 or wider, within the bound.
No kernel may reach another device: no remote copies, remote signals or barrier semaphores. Data moves between devices by JAX's collectives and lax.ppermute only.
A program may use at most 128 MiB of HBM per device.

```python
import jax
import jax.numpy as jnp
from jax import lax

R = 40
S_DEV = 2048
NE = 512
LEAF = 8
A_DEV = 64
S = 524288
LEAVES = 2048
NA = 4096
N_SRC = 64
N_GRP = 4


def leaf_layout(key):
    blocks = S // S_DEV
    position = jnp.arange(S_DEV, dtype=jnp.int32)[None, :]
    block_ids = jnp.arange(blocks, dtype=jnp.int32)[:, None]
    first_pick = jax.random.randint(jax.random.fold_in(key, 7), (blocks, S_DEV), 0, LEAF)
    second_pick = jax.random.randint(jax.random.fold_in(key, 11), (blocks, S_DEV), 0, LEAF)
    chosen = jnp.minimum(first_pick, second_pick).astype(jnp.int32)
    lone_box = jax.random.randint(jax.random.fold_in(key, 13), (blocks, 1), 0, LEAF).astype(jnp.int32)
    crowded = block_ids % 16 == 0
    chosen = jnp.where(crowded, lone_box, chosen).astype(jnp.int32)
    return jnp.where(position < LEAF, position, chosen).astype(jnp.int32)


def draw_leaf_box(key, part):
    return leaf_layout(key).reshape(S)


def draw_box_count(key, part):
    layout = leaf_layout(key)
    labels = jnp.arange(LEAF, dtype=jnp.int32)
    tallies = jnp.sum((layout[:, None, :] == labels[None, :, None]).astype(jnp.int32), axis=2)
    return tallies.reshape(LEAVES).astype(jnp.int32)


def level_of(rng, shape, pieces, least, largest):
    def one(dim, shards_of):
        draws = jax.random.uniform(jax.random.fold_in(jax.random.fold_in(rng, 6), dim), (shards_of,), jnp.float32, least / len(pieces), largest / len(pieces))
        return jnp.repeat(jnp.exp(draws), shape[dim] // shards_of).reshape((-1,) + (1,) * (len(shape) - dim - 1))

    level = one(*pieces[0])
    for cut in pieces[1:]:
        level = level * one(*cut)
    return level


def centred(own_key, dims, spread, limit, cuts=(), kind=jnp.bfloat16):
    result = spread * jax.random.normal(own_key, dims, jnp.float32)
    if cuts:
        result = result * level_of(own_key, dims, cuts, -0.22, 0.18)
    return jnp.clip(result, -limit, limit).astype(kind)


def setup_inputs(seed: int = 0) -> dict:
    splits = jax.random.split(jax.random.key(seed), 7)
    currents = centred(splits[0], (S, 2 * NE), 1.0, 6.0, ((0, 256),))
    leaf_basis = centred(splits[1], (2, R, S), 1.0, 6.0, ((2, 256),))
    leaf_box = draw_leaf_box(jax.random.fold_in(splits[6], 71), 0)
    box_count = draw_box_count(jax.random.fold_in(splits[6], 71), 0)
    merge_factor = centred(splits[4], (2, N_SRC * R, LEAVES * R), (2 * LEAF * R) ** -0.5, 0.25, ((2, 256),))
    angle_factor = centred(splits[5], (NA, N_GRP, 2, N_SRC * R), (2 * N_SRC * N_GRP * R) ** -0.5, 0.0390625, ((0, 64),))
    return dict(currents=currents, leaf_basis=leaf_basis, leaf_box=leaf_box, box_count=box_count, merge_factor=merge_factor, angle_factor=angle_factor)


def complex_apply(real_part, imag_part, right_side):
    half_width = right_side.shape[1] // 2
    first_part = jnp.dot(real_part, right_side, preferred_element_type=jnp.float32)
    second = jnp.dot(imag_part, right_side, preferred_element_type=jnp.float32)
    return jnp.concatenate([first_part[:, :half_width] - second[:, half_width:], first_part[:, half_width:] + second[:, :half_width]], axis=1)

def source_coefs(currents, leaf_basis, leaf_box, box_count, merge_factor):
    leaf_total = box_count.shape[0]
    rank_size = leaf_basis.shape[1]
    sources = currents.shape[0]
    labels = jnp.arange(leaf_total, dtype=jnp.int32)
    member = (leaf_box[None, :] == labels[:, None]).astype(jnp.float32)
    scaled = member * lax.rsqrt(box_count.astype(jnp.float32))[:, None]
    basis_wide = leaf_basis.astype(jnp.float32)
    left_real = (scaled[:, None, :] * basis_wide[0][None, :, :]).reshape(leaf_total * rank_size, sources).astype(jnp.bfloat16)
    left_imag = (scaled[:, None, :] * basis_wide[1][None, :, :]).reshape(leaf_total * rank_size, sources).astype(jnp.bfloat16)
    leaf_coefs = complex_apply(left_real, left_imag, currents).astype(jnp.bfloat16)
    return complex_apply(merge_factor[0], merge_factor[1], leaf_coefs).astype(jnp.bfloat16)

def angle_side(operands):
    factor, level_coefs = operands
    half_width = level_coefs.shape[2] // 2
    wide_coefs = level_coefs.astype(jnp.float32)
    first_part = jnp.einsum('aqk,qkc->ac', factor[:, :, 0].astype(jnp.float32), wide_coefs)
    second = jnp.einsum('aqk,qkc->ac', factor[:, :, 1].astype(jnp.float32), wide_coefs)
    return jnp.stack([first_part[:, :half_width] - second[:, half_width:], first_part[:, half_width:] + second[:, :half_width]], axis=1)

def reference(currents, leaf_basis, leaf_box, box_count, merge_factor, angle_factor):
    blocks = N_SRC * N_GRP
    rank_size = leaf_basis.shape[1]
    width_cols = currents.shape[1]

    def source_block(block_index):
        first_row = (block_index * S_DEV).astype(jnp.int32)
        first_leaf = (block_index * LEAF).astype(jnp.int32)
        block_currents = lax.dynamic_slice_in_dim(currents, first_row, S_DEV, 0)
        block_basis = lax.dynamic_slice_in_dim(leaf_basis, first_row, S_DEV, 2)
        block_boxes = lax.dynamic_slice_in_dim(leaf_box, first_row, S_DEV, 0)
        block_counts = lax.dynamic_slice_in_dim(box_count, first_leaf, LEAF, 0)
        block_merge = lax.dynamic_slice_in_dim(merge_factor, (first_leaf * rank_size).astype(jnp.int32), LEAF * rank_size, 2)
        return source_coefs(block_currents, block_basis, block_boxes, block_counts, block_merge)
    all_coefs = lax.map(source_block, jnp.arange(blocks, dtype=jnp.int32))
    grouped = all_coefs.reshape(N_SRC, N_GRP, N_SRC, rank_size, width_cols)
    grouped = grouped.transpose(2, 1, 0, 3, 4).reshape(N_SRC, N_GRP, N_SRC * rank_size, width_cols)
    factors = angle_factor.reshape(N_SRC, A_DEV, N_GRP, 2, N_SRC * rank_size)
    patterns = lax.map(angle_side, (factors, grouped))
    pattern = patterns.reshape(N_SRC * A_DEV, 2, width_cols // 2)
    intensity = pattern[:, 0] * pattern[:, 0] + pattern[:, 1] * pattern[:, 1]
    peak_value = lax.optimization_barrier(jnp.max(intensity, axis=0))
    return (intensity / (peak_value[None, :] + 1.0), peak_value)
```

```python
import jax
import jax.numpy as jnp
from jax import lax
from jax.experimental import pallas as pl
from jax.experimental.pallas import tpu as pltpu
from jax.sharding import Mesh
from jax.sharding import PartitionSpec as P


F32, BF16 = jnp.float32, jnp.bfloat16
NX, NZ, NC, NY = 4, 8, 2, 4
R, LEAF, S_DEV, NE, A = 40, 8, 2048, 512, 64
Q = NE // NY
SIZES = {"x": NX, "z": NZ, "c": NC, "y": NY}


def shift(v, axis, k):
    n = SIZES[axis]
    return lax.ppermute(v, axis, [(i, (i + k) % n) for i in range(n)])


def params(*sem):
    return pltpu.CompilerParams(dimension_semantics=sem, vmem_limit_bytes=56 * 2**20)


def leaf_kernel(count, box, basis, x_re, x_im, s_re, s_im, op):
    @pl.when(pl.program_id(0) == 0)
    def _():
        boxes = box[...]
        for part in range(2):
            wide = basis[part].astype(F32)
            for pair in range(LEAF // 2):
                rows = []
                for b in (2 * pair, 2 * pair + 1):
                    scale = lax.rsqrt(jnp.full((1, S_DEV), count[b].astype(F32), F32))
                    rows.append(wide * jnp.where(boxes == b, scale, 0.0))
                at = part * LEAF * R + pair * 2 * R
                op[at : at + 2 * R, :] = jnp.concatenate(rows, axis=0).astype(BF16)

    half = LEAF * R
    first = jnp.dot(op[...], x_re[...], preferred_element_type=F32)
    second = jnp.dot(op[...], x_im[...], preferred_element_type=F32)
    re = first[:half] - second[half:]
    im = second[:half] + first[half:]
    s_re[0] = re.astype(BF16)
    s_re[1] = (-im).astype(BF16)
    s_im[0] = im.astype(BF16)
    s_im[1] = re.astype(BF16)


def leaf(count, box, basis, currents):
    steps = 2
    width = NE // steps
    out = jax.ShapeDtypeStruct((2, LEAF * R, NE), BF16)
    return pl.pallas_call(
        leaf_kernel,
        grid_spec=pltpu.PrefetchScalarGridSpec(
            num_scalar_prefetch=1,
            grid=(steps,),
            in_specs=[
                pl.BlockSpec((1, S_DEV), lambda i, n: (0, 0)),
                pl.BlockSpec((2, R, S_DEV), lambda i, n: (0, 0, 0)),
                pl.BlockSpec((S_DEV, width), lambda i, n: (0, i)),
                pl.BlockSpec((S_DEV, width), lambda i, n: (0, i + steps)),
            ],
            out_specs=[pl.BlockSpec((2, LEAF * R, width), lambda i, n: (0, 0, i))] * 2,
            scratch_shapes=[pltpu.VMEM((2 * LEAF * R, S_DEV), BF16)],
        ),
        out_shape=[out, out],
        compiler_params=params("arbitrary"),
        name="leaf",
    )(count, box, basis, currents, currents)


def merge_kernel(me, m, s_re, s_im, keep, send):
    lhs = m[...].reshape(2 * LEAF * R, NZ * NC * R)
    dims = (((0,), (0,)), ((), ()))
    re = lax.dot_general(lhs, s_re[...].reshape(2 * LEAF * R, NE), dims, preferred_element_type=F32)
    im = lax.dot_general(lhs, s_im[...].reshape(2 * LEAF * R, NE), dims, preferred_element_type=F32)

    def write(own):
        for z in range(NZ):
            for c in range(NC):
                g = (z * NC + c) * R
                tile = jnp.concatenate([re[g : g + R], im[g : g + R]], axis=0).astype(BF16)
                if c == own:
                    keep[0, z] = tile
                else:
                    send[0, z] = tile

    for own in range(NC):
        pl.when(me[2] == own)(lambda own=own: write(own))


def merge(me, m, s_re, s_im):
    out = jax.ShapeDtypeStruct((NX, NZ, 2 * R, NE), BF16)
    return pl.pallas_call(
        merge_kernel,
        grid_spec=pltpu.PrefetchScalarGridSpec(
            num_scalar_prefetch=1,
            grid=(NX,),
            in_specs=[
                pl.BlockSpec((2, LEAF * R, NZ * NC * R), lambda i, n: (0, 0, i)),
                pl.BlockSpec((2, LEAF * R, NE), lambda i, n: (0, 0, 0)),
                pl.BlockSpec((2, LEAF * R, NE), lambda i, n: (0, 0, 0)),
            ],
            out_specs=[pl.BlockSpec((1, NZ, 2 * R, NE), lambda i, n: (i, 0, 0, 0))] * 2,
        ),
        out_shape=[out, out],
        compiler_params=params("arbitrary"),
        name="merge",
    )(me, m, s_re, s_im)


def factor_kernel(me, f, out):
    for z in range(NZ):
        both = f[0, z].astype(F32)
        first, second = both[:R], both[R:]
        own = jnp.where(me[2] == 0, first, second)
        other = jnp.where(me[2] == 0, second, first)
        rows = []
        for v in (own, other):
            rows += [v, jnp.concatenate([-v[:, A:], v[:, :A]], axis=1)]
        out[0, z] = jnp.concatenate(rows, axis=0).T.astype(BF16)


def factors(me, f):
    return pl.pallas_call(
        factor_kernel,
        grid_spec=pltpu.PrefetchScalarGridSpec(
            num_scalar_prefetch=1,
            grid=(NX,),
            in_specs=[pl.BlockSpec((1, NZ, 2 * R, 2 * A), lambda i, n: (i, 0, 0, 0))],
            out_specs=pl.BlockSpec((1, NZ, 2 * A, 4 * R), lambda i, n: (i, 0, 0, 0)),
        ),
        out_shape=jax.ShapeDtypeStruct((NX, NZ, 2 * A, 4 * R), BF16),
        compiler_params=params("arbitrary"),
        name="factors",
    )(me, f)


def pattern_kernel(me, keep, recv, fac, *refs):
    by_x, by_y, row = refs[:NX], refs[NX : NX + NY], refs[NX + NY]
    step = pl.program_id(0)

    def product(x):
        right = jnp.concatenate([keep[x, 0], recv[x, 0]], axis=0)
        return jnp.dot(fac[x, 0], right, preferred_element_type=F32).astype(BF16)

    @pl.when(step < NZ // 2)
    def _():
        for k in range(NX):
            by_x[k][0] = product(lax.rem(me[0] + k, NX))

    @pl.when(step >= NZ // 2)
    def _():
        for x in range(NX):
            row[...] = product(x)
            for k in range(NY):
                at = pl.multiple_of(lax.rem(me[3] + k, NY) * Q, Q)
                by_y[k][0, x] = row[:, pl.ds(at, Q)]


def pattern(me, keep, recv, fac):
    h = NZ // 2
    wide = pl.BlockSpec((1, 2 * A, NE), lambda i, n: (jnp.minimum(i, h - 1), 0, 0))
    cut = pl.BlockSpec((1, NX, 2 * A, Q), lambda i, n: (jnp.maximum(i - h, 0), 0, 0, 0))
    return pl.pallas_call(
        pattern_kernel,
        grid_spec=pltpu.PrefetchScalarGridSpec(
            num_scalar_prefetch=1,
            grid=(NZ,),
            in_specs=[
                pl.BlockSpec((NX, 1, 2 * R, NE), lambda i, n: (0, i, 0, 0)),
                pl.BlockSpec((NX, 1, 2 * R, NE), lambda i, n: (0, i, 0, 0)),
                pl.BlockSpec((NX, 1, 2 * A, 4 * R), lambda i, n: (0, i, 0, 0)),
            ],
            out_specs=[wide] * NX + [cut] * NY,
            scratch_shapes=[pltpu.VMEM((2 * A, NE), BF16)],
        ),
        out_shape=[jax.ShapeDtypeStruct((h, 2 * A, NE), BF16)] * NX
        + [jax.ShapeDtypeStruct((h, NX, 2 * A, Q), BF16)] * NY,
        compiler_params=params("arbitrary"),
        name="pattern",
    )(me, keep, recv, fac)


def second_kernel(me, *refs):
    wide, cut = refs[:NX], refs[NX : NX + NY]
    by_y, by_x = refs[NX + NY : NX + 2 * NY], refs[NX + 2 * NY :]
    for k in range(NY):
        at = pl.multiple_of(lax.rem(me[3] + k, NY) * Q, Q)
        by_y[k][0] = sum(r[0, :, pl.ds(at, Q)].astype(F32) for r in wide).astype(BF16)
    for k in range(NX):
        x = lax.rem(me[0] + k, NX)
        by_x[k][0] = sum(r[0, x].astype(F32) for r in cut).astype(BF16)


def second(me, wide, cut):
    h = NZ // 2
    out = jax.ShapeDtypeStruct((h, 2 * A, Q), BF16)
    spec = pl.BlockSpec((1, 2 * A, Q), lambda i, n: (i, 0, 0))
    return pl.pallas_call(
        second_kernel,
        grid_spec=pltpu.PrefetchScalarGridSpec(
            num_scalar_prefetch=1,
            grid=(h,),
            in_specs=[pl.BlockSpec((1, 2 * A, NE), lambda i, n: (i, 0, 0))] * NX
            + [pl.BlockSpec((1, NX, 2 * A, Q), lambda i, n: (i, 0, 0, 0))] * NY,
            out_specs=[spec] * (NY + NX),
        ),
        out_shape=[out] * (NY + NX),
        compiler_params=params("arbitrary"),
        name="second",
    )(me, *wide, *cut)


def third_kernel(*refs):
    out = refs[-1]
    h = NZ // 2
    out[:h] = sum(r[...].astype(F32) for r in refs[:NY]).astype(BF16)
    out[h:] = sum(r[...].astype(F32) for r in refs[NY:-1]).astype(BF16)


def third(parts):
    return pl.pallas_call(
        third_kernel,
        out_shape=jax.ShapeDtypeStruct((NZ, 2 * A, Q), BF16),
        name="third",
    )(*parts)


def last_kernel(parts, intensity, top):
    total = jnp.sum(parts[...].astype(F32), axis=0)
    value = total[:A] * total[:A] + total[A:] * total[A:]
    intensity[...] = value
    top[...] = jnp.max(value, axis=0, keepdims=True)


def last(parts):
    return pl.pallas_call(
        last_kernel,
        out_shape=[jax.ShapeDtypeStruct((A, Q), F32), jax.ShapeDtypeStruct((1, Q), F32)],
        name="last",
    )(parts)


def body(currents, leaf_basis, leaf_box, box_count, merge_factor, angle_factor):
    me = jnp.stack([lax.axis_index(a).astype(jnp.int32) for a in ("x", "z", "c", "y")])
    own = lax.dynamic_index_in_dim(angle_factor, lax.axis_index("y"), 1, keepdims=False)
    own = own.transpose(2, 1, 0).reshape(NX * NZ, NC * R, 2 * A)
    gathered = lax.all_to_all(own, ("x", "z"), 0, 0, tiled=True)
    fac = factors(me, gathered.reshape(NX, NZ, NC * R, 2 * A))
    s_re, s_im = leaf(box_count, leaf_box.reshape(1, S_DEV), leaf_basis, currents)
    keep, send = merge(me, merge_factor.swapaxes(1, 2), s_re, s_im)
    recv = shift(send, "c", 1)
    cuts = pattern(me, keep, recv, fac)
    wide = [cuts[0]] + [shift(cuts[k], "x", k) for k in range(1, NX)]
    cut = [cuts[NX]] + [shift(cuts[NX + k], "y", k) for k in range(1, NY)]
    cuts = second(me, wide, cut)
    parts = [cuts[0]] + [shift(cuts[k], "y", k) for k in range(1, NY)]
    parts += [cuts[NY]] + [shift(cuts[NY + k], "x", k) for k in range(1, NX)]
    parts = lax.all_to_all(third(parts), "z", 0, 0, tiled=True)
    intensity, top = last(parts)
    tops = jnp.broadcast_to(top[None], (NX * NZ * NC, 1, Q))
    tops = lax.all_to_all(tops, ("x", "z", "c"), 0, 0, tiled=True)
    peak = jnp.max(tops, axis=(0, 1))
    return intensity / (peak[None, :] + 1.0), peak


def solution(mesh):
    split = Mesh(mesh.devices.reshape(NX, NZ, NC, NY), ("x", "z", "c", "y"))
    src, every = ("x", "z", "c"), ("x", "z", "c", "y")
    in_specs = (
        P(every, None),
        P(None, None, every),
        P(every),
        P(every),
        P(None, None, every),
        P(src, None, None, None),
    )
    out_specs = (P(src, "y"), P("y"))
    return jax.shard_map(body, mesh=split, in_specs=in_specs, out_specs=out_specs, check_vma=False)
```

```python
import jax
import jax.numpy as jnp
from jax import lax
from jax.experimental import pallas as pl
from jax.experimental.pallas import tpu as pltpu
from jax.sharding import Mesh
from jax.sharding import PartitionSpec as P


F32, BF16 = jnp.float32, jnp.bfloat16
NX, NZ, NC, NY = 4, 8, 2, 4
R, LEAF, S_DEV, NE, A = 40, 8, 2048, 512, 64
Q = NE // NY
LEAF_STEPS = 2
ZS = 2
SIZES = {"x": NX, "z": NZ, "c": NC, "y": NY}


def shift(v, axis, k):
    n = SIZES[axis]
    return lax.ppermute(v, axis, [(i, (i + k) % n) for i in range(n)])


def params(*sem):
    return pltpu.CompilerParams(dimension_semantics=sem, vmem_limit_bytes=56 * 2**20)


def source_kernel(count, me, box, basis, x_re, x_im, m, keep, send, op, stacked):
    step = pl.program_id(0)
    half = LEAF * R

    @pl.when(step == 0)
    def _():
        boxes = box[...]
        for part in range(2):
            wide = basis[part].astype(F32)
            for pair in range(LEAF // 2):
                rows = []
                for b in (2 * pair, 2 * pair + 1):
                    scale = lax.rsqrt(jnp.full((1, S_DEV), count[b].astype(F32), F32))
                    rows.append(wide * jnp.where(boxes == b, scale, 0.0))
                at = part * half + pair * 2 * R
                op[at : at + 2 * R, :] = jnp.concatenate(rows, axis=0).astype(BF16)

    width = NE // LEAF_STEPS
    for k in range(LEAF_STEPS):

        @pl.when(step == k)
        def _(k=k):
            first = jnp.dot(op[...], x_re[...], preferred_element_type=F32)
            second = jnp.dot(op[...], x_im[...], preferred_element_type=F32)
            re = first[:half] - second[half:]
            im = second[:half] + first[half:]
            left, right = pl.ds(k * width, width), pl.ds(NE + k * width, width)
            stacked[:half, left] = re.astype(BF16)
            stacked[half:, left] = (-im).astype(BF16)
            stacked[:half, right] = im.astype(BF16)
            stacked[half:, right] = re.astype(BF16)

    @pl.when(step >= LEAF_STEPS)
    def _():
        rows = m[...].reshape(2 * half, NZ * NC * R).T
        out = jnp.dot(rows, stacked[...], preferred_element_type=F32)

        def write(own):
            for z in range(NZ):
                for c in range(NC):
                    g = (z * NC + c) * R
                    tile = [out[g : g + R, :NE], out[g : g + R, NE:]]
                    (keep if c == own else send)[0, z] = jnp.concatenate(tile, axis=0).astype(BF16)

        for own in range(NC):
            pl.when(me[2] == own)(lambda own=own: write(own))


def source(count, me, box, basis, currents, m):
    out = jax.ShapeDtypeStruct((NX, NZ, 2 * R, NE), BF16)
    width = NE // LEAF_STEPS

    def leaf_at(i):
        return jnp.minimum(i, LEAF_STEPS - 1)

    def merge_at(i):
        return jnp.maximum(i - LEAF_STEPS, 0)

    return pl.pallas_call(
        source_kernel,
        grid_spec=pltpu.PrefetchScalarGridSpec(
            num_scalar_prefetch=2,
            grid=(LEAF_STEPS + NX,),
            in_specs=[
                pl.BlockSpec((1, S_DEV), lambda i, *n: (0, 0)),
                pl.BlockSpec((2, R, S_DEV), lambda i, *n: (0, 0, 0)),
                pl.BlockSpec((S_DEV, width), lambda i, *n: (0, leaf_at(i))),
                pl.BlockSpec((S_DEV, width), lambda i, *n: (0, leaf_at(i) + LEAF_STEPS)),
                pl.BlockSpec((2, LEAF * R, NZ * NC * R), lambda i, *n: (0, 0, merge_at(i))),
            ],
            out_specs=[pl.BlockSpec((1, NZ, 2 * R, NE), lambda i, *n: (merge_at(i), 0, 0, 0))] * 2,
            scratch_shapes=[
                pltpu.VMEM((2 * LEAF * R, S_DEV), BF16),
                pltpu.VMEM((2 * LEAF * R, 2 * NE), BF16),
            ],
        ),
        out_shape=[out, out],
        compiler_params=params("arbitrary"),
        name="source",
    )(count, me, box, basis, currents, currents, m)


def turn_kernel(f, out):
    out[...] = f[...].T


def turn(f):
    return pl.pallas_call(
        turn_kernel, out_shape=jax.ShapeDtypeStruct(f.shape[::-1], f.dtype), name="turn"
    )(f)


def factor_kernel(me, f, out):
    for z in range(NZ):
        both = f[0, z].astype(F32)
        first, second = both[:R], both[R:]
        own = jnp.where(me[2] == 0, first, second)
        other = jnp.where(me[2] == 0, second, first)
        rows = []
        for v in (own, other):
            rows += [v, jnp.concatenate([-v[:, A:], v[:, :A]], axis=1)]
        out[0, z] = jnp.concatenate(rows, axis=0).T.astype(BF16)


def factors(me, f):
    return pl.pallas_call(
        factor_kernel,
        grid_spec=pltpu.PrefetchScalarGridSpec(
            num_scalar_prefetch=1,
            grid=(NX,),
            in_specs=[pl.BlockSpec((1, NZ, 2 * R, 2 * A), lambda i, n: (i, 0, 0, 0))],
            out_specs=pl.BlockSpec((1, NZ, 2 * A, 4 * R), lambda i, n: (i, 0, 0, 0)),
        ),
        out_shape=jax.ShapeDtypeStruct((NX, NZ, 2 * A, 4 * R), BF16),
        compiler_params=params("arbitrary"),
        name="factors",
    )(me, f)


def pattern_kernel(me, keep, recv, fac, *refs):
    by_x, by_y, row = refs[:NX], refs[NX : NX + NY], refs[NX + NY]
    step = pl.program_id(0)

    def product(x, z):
        right = jnp.concatenate([keep[x, z], recv[x, z]], axis=0)
        return jnp.dot(fac[x, z], right, preferred_element_type=F32).astype(BF16)

    @pl.when(step < NZ // 2 // ZS)
    def _():
        for z in range(ZS):
            pieces = [product(lax.rem(me[0] + k, NX), z) for k in range(NX)]
            for k in range(NX):
                by_x[k][z] = pieces[k]

    @pl.when(step >= NZ // 2 // ZS)
    def _():
        for z in range(ZS):
            for x in range(NX):
                row[z, x] = product(x, z)
        for k in range(NY):
            at = pl.multiple_of(lax.rem(me[3] + k, NY) * Q, Q)
            by_y[k][...] = row[:, :, :, pl.ds(at, Q)]


def pattern(me, keep, recv, fac):
    h = NZ // 2 // ZS
    wide = pl.BlockSpec((ZS, 2 * A, NE), lambda i, n: (jnp.minimum(i, h - 1), 0, 0))
    cut = pl.BlockSpec((ZS, NX, 2 * A, Q), lambda i, n: (jnp.maximum(i - h, 0), 0, 0, 0))
    return pl.pallas_call(
        pattern_kernel,
        grid_spec=pltpu.PrefetchScalarGridSpec(
            num_scalar_prefetch=1,
            grid=(NZ // ZS,),
            in_specs=[
                pl.BlockSpec((NX, ZS, 2 * R, NE), lambda i, n: (0, i, 0, 0)),
                pl.BlockSpec((NX, ZS, 2 * R, NE), lambda i, n: (0, i, 0, 0)),
                pl.BlockSpec((NX, ZS, 2 * A, 4 * R), lambda i, n: (0, i, 0, 0)),
            ],
            out_specs=[wide] * NX + [cut] * NY,
            scratch_shapes=[pltpu.VMEM((ZS, NX, 2 * A, NE), BF16)],
        ),
        out_shape=[jax.ShapeDtypeStruct((NZ // 2, 2 * A, NE), BF16)] * NX
        + [jax.ShapeDtypeStruct((NZ // 2, NX, 2 * A, Q), BF16)] * NY,
        compiler_params=params("arbitrary"),
        name="pattern",
    )(me, keep, recv, fac)


def second_kernel(me, *refs):
    wide, cut = refs[:NX], refs[NX : NX + NY]
    by_y, by_x = refs[NX + NY : NX + 2 * NY], refs[NX + 2 * NY :]
    for z in range(NZ // 2):
        for k in range(NY):
            at = pl.multiple_of(lax.rem(me[3] + k, NY) * Q, Q)
            by_y[k][z] = sum(r[z, :, pl.ds(at, Q)].astype(F32) for r in wide).astype(BF16)
        for k in range(NX):
            x = lax.rem(me[0] + k, NX)
            by_x[k][z] = sum(r[z, x].astype(F32) for r in cut).astype(BF16)


def second(me, wide, cut):
    out = jax.ShapeDtypeStruct((NZ // 2, 2 * A, Q), BF16)
    vmem = pl.BlockSpec(memory_space=pltpu.VMEM)
    return pl.pallas_call(
        second_kernel,
        in_specs=[pl.BlockSpec(memory_space=pltpu.SMEM)] + [vmem] * (NX + NY),
        out_specs=[vmem] * (NY + NX),
        out_shape=[out] * (NY + NX),
        compiler_params=params(),
        name="second",
    )(me, *wide, *cut)


def third_kernel(*refs):
    out = refs[-1]
    h = NZ // 2
    out[:h] = sum(r[...].astype(F32) for r in refs[:NY]).astype(BF16)
    out[h:] = sum(r[...].astype(F32) for r in refs[NY:-1]).astype(BF16)


def third(parts):
    return pl.pallas_call(
        third_kernel,
        out_shape=jax.ShapeDtypeStruct((NZ, 2 * A, Q), BF16),
        name="third",
    )(*parts)


def last_kernel(parts, intensity, top):
    total = jnp.sum(parts[...].astype(F32), axis=0)
    value = total[:A] * total[:A] + total[A:] * total[A:]
    intensity[...] = value
    top[...] = jnp.max(value, axis=0, keepdims=True)


def last(parts):
    return pl.pallas_call(
        last_kernel,
        out_shape=[jax.ShapeDtypeStruct((A, Q), F32), jax.ShapeDtypeStruct((1, Q), F32)],
        name="last",
    )(parts)


def body(currents, leaf_basis, leaf_box, box_count, merge_factor, angle_factor):
    me = jnp.stack([lax.axis_index(a).astype(jnp.int32) for a in ("x", "z", "c", "y")])
    own = lax.dynamic_index_in_dim(angle_factor, lax.axis_index("y"), 1, keepdims=False)
    own = turn(own.transpose(1, 0, 2).reshape(2 * A, NX * NZ * NC * R))
    own = own.reshape(NX * NZ, NC * R, 2 * A)
    spread = lax.all_to_all(own, ("x", "z"), 0, 0, tiled=True)
    box = leaf_box.reshape(1, S_DEV)
    coefs = merge_factor.swapaxes(1, 2)
    keep, send = source(box_count, me, box, leaf_basis, currents, coefs)
    fac = factors(me, spread.reshape(NX, NZ, NC * R, 2 * A))
    recv = shift(send, "c", 1)
    cuts = pattern(me, keep, recv, fac)
    wide = [cuts[0]] + [shift(cuts[k], "x", k) for k in range(1, NX)]
    cut = [cuts[NX]] + [shift(cuts[NX + k], "y", k) for k in range(1, NY)]
    cuts = second(me, wide, cut)
    parts = [cuts[0]] + [shift(cuts[k], "y", k) for k in range(1, NY)]
    parts += [cuts[NY]] + [shift(cuts[NY + k], "x", k) for k in range(1, NX)]
    parts = lax.all_to_all(third(parts), "z", 0, 0, tiled=True)
    intensity, top = last(parts)
    tops = jnp.broadcast_to(top[None], (NX * NZ * NC, 1, Q))
    tops = lax.all_to_all(tops, ("x", "z", "c"), 0, 0, tiled=True)
    peak = jnp.max(tops, axis=(0, 1))
    return intensity / (peak[None, :] + 1.0), peak


def solution(mesh):
    split = Mesh(mesh.devices.reshape(NX, NZ, NC, NY), ("x", "z", "c", "y"))
    src, every = ("x", "z", "c"), ("x", "z", "c", "y")
    in_specs = (
        P(every, None),
        P(None, None, every),
        P(every),
        P(every),
        P(None, None, every),
        P(src, None, None, None),
    )
    out_specs = (P(src, "y"), P("y"))
    return jax.shard_map(body, mesh=split, in_specs=in_specs, out_specs=out_specs, check_vma=False)
```

```python
import jax
import jax.numpy as jnp
from jax import lax
from jax.experimental import pallas as pl
from jax.experimental.pallas import tpu as pltpu
from jax.sharding import Mesh
from jax.sharding import PartitionSpec as P


F32, BF16 = jnp.float32, jnp.bfloat16
NX, NZ, NC, NY = 4, 8, 2, 4
R, LEAF, S_DEV, NE, A = 40, 8, 2048, 512, 64
Q = NE // NY
LEAF_STEPS = 2
CHUNKS = 2
ORDER = (2, 1, 3)
SIZES = {"x": NX, "z": NZ, "c": NC, "y": NY}


def shift(v, axis, k):
    n = SIZES[axis]
    return lax.ppermute(v, axis, [(i, (i + k) % n) for i in range(n)])


def params(*sem):
    return pltpu.CompilerParams(dimension_semantics=sem, vmem_limit_bytes=56 * 2**20)


def source_kernel(count, me, box, basis, x_re, x_im, m, keep, send, op, stacked):
    step = pl.program_id(0)
    half = LEAF * R

    @pl.when(step == 0)
    def _():
        boxes = box[...]
        for part in range(2):
            wide = basis[part].astype(F32)
            for pair in range(LEAF // 2):
                rows = []
                for b in (2 * pair, 2 * pair + 1):
                    scale = lax.rsqrt(jnp.full((1, S_DEV), count[b].astype(F32), F32))
                    rows.append(wide * jnp.where(boxes == b, scale, 0.0))
                at = part * half + pair * 2 * R
                op[at : at + 2 * R, :] = jnp.concatenate(rows, axis=0).astype(BF16)

    width = NE // LEAF_STEPS
    for k in range(LEAF_STEPS):

        @pl.when(step == k)
        def _(k=k):
            first = jnp.dot(op[...], x_re[...], preferred_element_type=F32)
            second = jnp.dot(op[...], x_im[...], preferred_element_type=F32)
            re = first[:half] - second[half:]
            im = second[:half] + first[half:]
            left, right = pl.ds(k * width, width), pl.ds(NE + k * width, width)
            stacked[:half, left] = re.astype(BF16)
            stacked[half:, left] = (-im).astype(BF16)
            stacked[:half, right] = im.astype(BF16)
            stacked[half:, right] = re.astype(BF16)

    @pl.when(step >= LEAF_STEPS)
    def _():
        rows = m[...].reshape(2 * half, NZ * NC * R).T
        out = jnp.dot(rows, stacked[...], preferred_element_type=F32)

        def write(own):
            for z in range(NZ):
                for c in range(NC):
                    g = (z * NC + c) * R
                    tile = [out[g : g + R, :NE], out[g : g + R, NE:]]
                    (keep if c == own else send)[0, z] = jnp.concatenate(tile, axis=0).astype(BF16)

        for own in range(NC):
            pl.when(me[2] == own)(lambda own=own: write(own))


def source(count, me, box, basis, currents, m):
    out = jax.ShapeDtypeStruct((NX, NZ, 2 * R, NE), BF16)
    width = NE // LEAF_STEPS

    def leaf_at(i):
        return jnp.minimum(i, LEAF_STEPS - 1)

    def merge_at(i):
        return jnp.maximum(i - LEAF_STEPS, 0)

    return pl.pallas_call(
        source_kernel,
        grid_spec=pltpu.PrefetchScalarGridSpec(
            num_scalar_prefetch=2,
            grid=(LEAF_STEPS + NX,),
            in_specs=[
                pl.BlockSpec((1, S_DEV), lambda i, *n: (0, 0)),
                pl.BlockSpec((2, R, S_DEV), lambda i, *n: (0, 0, 0)),
                pl.BlockSpec((S_DEV, width), lambda i, *n: (0, leaf_at(i))),
                pl.BlockSpec((S_DEV, width), lambda i, *n: (0, leaf_at(i) + LEAF_STEPS)),
                pl.BlockSpec((2, LEAF * R, NZ * NC * R), lambda i, *n: (0, 0, merge_at(i))),
            ],
            out_specs=[pl.BlockSpec((1, NZ, 2 * R, NE), lambda i, *n: (merge_at(i), 0, 0, 0))] * 2,
            scratch_shapes=[
                pltpu.VMEM((2 * LEAF * R, S_DEV), BF16),
                pltpu.VMEM((2 * LEAF * R, 2 * NE), BF16),
            ],
        ),
        out_shape=[out, out],
        compiler_params=params("arbitrary"),
        name="source",
    )(count, me, box, basis, currents, currents, m)


def turn_kernel(me, f, out):
    wide = f[:, 0].astype(F32)
    out[...] = jnp.concatenate([wide[:, 0], wide[:, 1]], axis=0).astype(BF16).T


def turn(me, factor):
    steps, columns = 4, factor.shape[3]
    width = columns // steps
    return pl.pallas_call(
        turn_kernel,
        grid_spec=pltpu.PrefetchScalarGridSpec(
            num_scalar_prefetch=1,
            grid=(steps,),
            in_specs=[pl.BlockSpec((A, 1, 2, width), lambda i, n: (0, n[3], 0, i))],
            out_specs=pl.BlockSpec((width, 2 * A), lambda i, n: (i, 0)),
        ),
        out_shape=jax.ShapeDtypeStruct((columns, 2 * A), BF16),
        compiler_params=params("arbitrary"),
        name="turn",
    )(me, factor)


def pattern_kernel(me, keep, recv, fac, *refs):
    by_x, by_y, row = refs[:NX], refs[NX : NX + NY], refs[NX + NY]
    first = me[2] == 0

    def product(x, part):
        both = fac[x, part, 0].astype(F32)
        turned = jnp.concatenate([-both[:, A:], both[:, :A]], axis=1)
        left = jnp.concatenate([both[:R], turned[:R], both[R:], turned[R:]], axis=0).astype(BF16)
        own, other = keep[x, part, 0], recv[x, part, 0]
        right = jnp.concatenate(
            [jnp.where(first, own, other), jnp.where(first, other, own)], axis=0
        )
        return jnp.dot(left.T, right, preferred_element_type=F32).astype(BF16)

    pieces = [product(lax.rem(me[0] + k, NX), 0) for k in range(NX)]
    for k in range(NX):
        by_x[k][0] = pieces[k]
    for x in range(NX):
        row[x] = product(x, 1)
    for k in range(NY):
        at = pl.multiple_of(lax.rem(me[3] + k, NY) * Q, Q)
        by_y[k][0] = row[:, :, pl.ds(at, Q)]


def pattern(me, keep, recv, fac, chunk):
    steps = NZ // 2 // CHUNKS

    def halves(v):
        return v.reshape((NX, 2, NZ // 2) + v.shape[2:])

    def at(i, n):
        return (0, 0, chunk * steps + i, 0, 0)

    wide = pl.BlockSpec((1, 2 * A, NE), lambda i, n: (i, 0, 0))
    cut = pl.BlockSpec((1, NX, 2 * A, Q), lambda i, n: (i, 0, 0, 0))
    return pl.pallas_call(
        pattern_kernel,
        grid_spec=pltpu.PrefetchScalarGridSpec(
            num_scalar_prefetch=1,
            grid=(steps,),
            in_specs=[
                pl.BlockSpec((NX, 2, 1, 2 * R, NE), at),
                pl.BlockSpec((NX, 2, 1, 2 * R, NE), at),
                pl.BlockSpec((NX, 2, 1, 2 * R, 2 * A), at),
            ],
            out_specs=[wide] * NX + [cut] * NY,
            scratch_shapes=[pltpu.VMEM((NX, 2 * A, NE), BF16)],
        ),
        out_shape=[jax.ShapeDtypeStruct((steps, 2 * A, NE), BF16)] * NX
        + [jax.ShapeDtypeStruct((steps, NX, 2 * A, Q), BF16)] * NY,
        compiler_params=params("arbitrary"),
        name="pattern",
    )(me, halves(keep), halves(recv), halves(fac))


def second_kernel(me, *refs):
    wide, cut = refs[:NX], refs[NX : NX + NY]
    by_y, by_x = refs[-NY - NX : -NX], refs[-NX:]
    for z in range(NZ // 2 // CHUNKS):
        for k in range(NY):
            at = pl.multiple_of(lax.rem(me[3] + k, NY) * Q, Q)
            by_y[k][z] = sum(r[z, :, pl.ds(at, Q)].astype(F32) for r in wide).astype(BF16)
        for k in range(NX):
            x = lax.rem(me[0] + k, NX)
            by_x[k][z] = sum(r[z, x].astype(F32) for r in cut).astype(BF16)


def second(me, wide, cut, chunk, earlier):
    rows = NZ // 2 // CHUNKS
    pieces = NY + NX
    out = jax.ShapeDtypeStruct((NZ // 2, 2 * A, Q), BF16)
    return pl.pallas_call(
        second_kernel,
        grid_spec=pltpu.PrefetchScalarGridSpec(
            num_scalar_prefetch=1,
            grid=(1,),
            in_specs=[pl.BlockSpec((rows, 2 * A, NE), lambda i, n: (0, 0, 0))] * NX
            + [pl.BlockSpec((rows, NX, 2 * A, Q), lambda i, n: (0, 0, 0, 0))] * NY
            + [pl.BlockSpec(memory_space=pl.ANY)] * len(earlier),
            out_specs=[pl.BlockSpec((rows, 2 * A, Q), lambda i, n: (chunk, 0, 0))] * pieces,
        ),
        out_shape=[out] * pieces,
        input_output_aliases={1 + pieces + i: i for i in range(len(earlier))},
        compiler_params=params("arbitrary"),
        name="second",
    )(me, *wide, *cut, *earlier)


def third_kernel(*refs):
    out = refs[-1]
    h = NZ // 2
    out[:h] = sum(r[...].astype(F32) for r in refs[:NY]).astype(BF16)
    out[h:] = sum(r[...].astype(F32) for r in refs[NY:-1]).astype(BF16)


def third(parts):
    return pl.pallas_call(
        third_kernel,
        out_shape=jax.ShapeDtypeStruct((NZ, 2 * A, Q), BF16),
        name="third",
    )(*parts)


def last_kernel(parts, intensity, top):
    total = jnp.sum(parts[...].astype(F32), axis=0)
    value = total[:A] * total[:A] + total[A:] * total[A:]
    intensity[...] = value
    top[...] = jnp.broadcast_to(jnp.max(value, axis=0, keepdims=True)[None], top.shape)


def last(parts):
    return pl.pallas_call(
        last_kernel,
        out_shape=[
            jax.ShapeDtypeStruct((A, Q), F32),
            jax.ShapeDtypeStruct((NX * NZ * NC, 1, Q), F32),
        ],
        name="last",
    )(parts)


def exchange(first, second, axes):
    firsts, seconds = [first[0]] + [None] * (NX - 1), [second[0]] + [None] * (NY - 1)
    for k in ORDER:
        firsts[k] = shift(first[k], axes[0], k)
        seconds[k] = shift(second[k], axes[1], k)
    return firsts, seconds


def body(currents, leaf_basis, leaf_box, box_count, merge_factor, angle_factor):
    me = jnp.stack([lax.axis_index(a).astype(jnp.int32) for a in ("x", "z", "c", "y")])
    own = turn(me, angle_factor)
    own = own.reshape(NX * NZ, NC * R, 2 * A)
    spread = lax.all_to_all(own, ("x", "z"), 0, 0, tiled=True)
    box = leaf_box.reshape(1, S_DEV)
    coefs = merge_factor.swapaxes(1, 2)
    keep, send = source(box_count, me, box, leaf_basis, currents, coefs)
    fac = spread.reshape(NX, NZ, NC * R, 2 * A)
    recv = shift(send, "c", 1)
    sent = []
    for chunk in range(CHUNKS):
        pieces = pattern(me, keep, recv, fac, chunk)
        sent.append(exchange(pieces[:NX], pieces[NX:], ("x", "y")))
    pieces = []
    for chunk in range(CHUNKS):
        pieces = second(me, *sent[chunk], chunk, pieces)
    firsts, seconds = exchange(pieces[:NY], pieces[NY:], ("y", "x"))
    parts = lax.all_to_all(third(firsts + seconds), "z", 0, 0, tiled=True)
    intensity, tops = last(parts)
    tops = lax.all_to_all(tops, ("x", "z", "c"), 0, 0, tiled=True)
    peak = jnp.max(tops, axis=(0, 1))
    return intensity / (peak[None, :] + 1.0), peak


def solution(mesh):
    split = Mesh(mesh.devices.reshape(NX, NZ, NC, NY), ("x", "z", "c", "y"))
    src, every = ("x", "z", "c"), ("x", "z", "c", "y")
    in_specs = (
        P(every, None),
        P(None, None, every),
        P(every),
        P(every),
        P(None, None, every),
        P(src, None, None, None),
    )
    out_specs = (P(src, "y"), P("y"))
    return jax.shard_map(body, mesh=split, in_specs=in_specs, out_specs=out_specs, check_vma=False)
```

```python
import jax
import jax.numpy as jnp
from jax import lax
from jax.experimental import pallas as pl
from jax.experimental.pallas import tpu as pltpu
from jax.sharding import Mesh
from jax.sharding import PartitionSpec as P


F32, BF16 = jnp.float32, jnp.bfloat16
NX, NZ, NC, NY = 4, 8, 2, 4
R, LEAF, S_DEV, NE, A = 40, 8, 2048, 512, 64
Q = NE // NY
LEAF_STEPS = 2
CHUNKS = 2
ORDER = (1, 3, 2)
SIZES = {"x": NX, "z": NZ, "c": NC, "y": NY}


def shift(v, axis, k):
    n = SIZES[axis]
    return lax.ppermute(v, axis, [(i, (i + k) % n) for i in range(n)])


def params(*sem, mb=16):
    return pltpu.CompilerParams(dimension_semantics=sem, vmem_limit_bytes=mb * 2**20)


def source_kernel(count, me, box, basis, x_re, x_im, m, keep, send, op, stacked):
    step = pl.program_id(0)
    half = LEAF * R

    @pl.when(step == 0)
    def _():
        boxes = box[...]
        for part in range(2):
            wide = basis[part].astype(F32)
            for pair in range(LEAF // 2):
                rows = []
                for b in (2 * pair, 2 * pair + 1):
                    scale = lax.rsqrt(jnp.full((1, S_DEV), count[b].astype(F32), F32))
                    rows.append(wide * jnp.where(boxes == b, scale, 0.0))
                at = part * half + pair * 2 * R
                op[at : at + 2 * R, :] = jnp.concatenate(rows, axis=0).astype(BF16)

    width = NE // LEAF_STEPS
    for k in range(LEAF_STEPS):

        @pl.when(step == k)
        def _(k=k):
            first = jnp.dot(op[...], x_re[...], preferred_element_type=F32)
            second = jnp.dot(op[...], x_im[...], preferred_element_type=F32)
            re = first[:half] - second[half:]
            im = second[:half] + first[half:]
            left, right = pl.ds(k * width, width), pl.ds(NE + k * width, width)
            stacked[:half, left] = re.astype(BF16)
            stacked[half:, left] = (-im).astype(BF16)
            stacked[:half, right] = im.astype(BF16)
            stacked[half:, right] = re.astype(BF16)

    @pl.when(step >= LEAF_STEPS)
    def _():
        rows = m[...].reshape(2 * half, NZ * NC * R).T
        out = jnp.dot(rows, stacked[...], preferred_element_type=F32)

        def write(own):
            for z in range(NZ):
                for c in range(NC):
                    g = (z * NC + c) * R
                    tile = [out[g : g + R, :NE], out[g : g + R, NE:]]
                    (keep if c == own else send)[0, z] = jnp.concatenate(tile, axis=0).astype(BF16)

        for own in range(NC):
            pl.when(me[2] == own)(lambda own=own: write(own))


def source(count, me, box, basis, currents, m):
    out = jax.ShapeDtypeStruct((NX, NZ, 2 * R, NE), BF16)
    width = NE // LEAF_STEPS

    def leaf_at(i):
        return jnp.minimum(i, LEAF_STEPS - 1)

    def merge_at(i):
        return jnp.maximum(i - LEAF_STEPS, 0)

    return pl.pallas_call(
        source_kernel,
        grid_spec=pltpu.PrefetchScalarGridSpec(
            num_scalar_prefetch=2,
            grid=(LEAF_STEPS + NX,),
            in_specs=[
                pl.BlockSpec((1, S_DEV), lambda i, *n: (0, 0)),
                pl.BlockSpec((2, R, S_DEV), lambda i, *n: (0, 0, 0)),
                pl.BlockSpec((S_DEV, width), lambda i, *n: (0, leaf_at(i))),
                pl.BlockSpec((S_DEV, width), lambda i, *n: (0, leaf_at(i) + LEAF_STEPS)),
                pl.BlockSpec((2, LEAF * R, NZ * NC * R), lambda i, *n: (0, 0, merge_at(i))),
            ],
            out_specs=[pl.BlockSpec((1, NZ, 2 * R, NE), lambda i, *n: (merge_at(i), 0, 0, 0))] * 2,
            scratch_shapes=[
                pltpu.VMEM((2 * LEAF * R, S_DEV), BF16),
                pltpu.VMEM((2 * LEAF * R, 2 * NE), BF16),
            ],
        ),
        out_shape=[out, out],
        compiler_params=params("arbitrary", mb=28),
        name="source",
    )(count, me, box, basis, currents, currents, m)


def turn_kernel(me, f, out):
    wide = f[:, 0].astype(F32)
    out[...] = jnp.concatenate([wide[:, 0], wide[:, 1]], axis=0).astype(BF16).T


def turn(me, factor):
    steps, columns = 4, factor.shape[3]
    width = columns // steps
    return pl.pallas_call(
        turn_kernel,
        grid_spec=pltpu.PrefetchScalarGridSpec(
            num_scalar_prefetch=1,
            grid=(steps,),
            in_specs=[pl.BlockSpec((A, 1, 2, width), lambda i, n: (0, n[3], 0, i))],
            out_specs=pl.BlockSpec((width, 2 * A), lambda i, n: (i, 0)),
        ),
        out_shape=jax.ShapeDtypeStruct((columns, 2 * A), BF16),
        compiler_params=params("arbitrary"),
        name="turn",
    )(me, factor)


def pattern_kernel(me, keep, recv, fac, *refs):
    by_x, by_y, row = refs[:NX], refs[NX : NX + NY], refs[NX + NY]
    first = me[2] == 0

    def product(x, part):
        both = fac[x, part, 0].astype(F32)
        turned = jnp.concatenate([-both[:, A:], both[:, :A]], axis=1)
        left = jnp.concatenate([both[:R], turned[:R], both[R:], turned[R:]], axis=0).astype(BF16)
        own, other = keep[x, part, 0], recv[x, part, 0]
        right = jnp.concatenate(
            [jnp.where(first, own, other), jnp.where(first, other, own)], axis=0
        )
        return jnp.dot(left.T, right, preferred_element_type=F32).astype(BF16)

    pieces = [product(lax.rem(me[0] + k, NX), 0) for k in range(NX)]
    for k in range(NX):
        by_x[k][0] = pieces[k]
    for x in range(NX):
        row[x] = product(x, 1)
    for k in range(NY):
        at = pl.multiple_of(lax.rem(me[3] + k, NY) * Q, Q)
        by_y[k][0] = row[:, :, pl.ds(at, Q)]


def pattern(me, keep, recv, fac, chunk):
    steps = NZ // 2 // CHUNKS

    def halves(v):
        return v.reshape((NX, 2, NZ // 2) + v.shape[2:])

    def at(i, n):
        return (0, 0, chunk * steps + i, 0, 0)

    wide = pl.BlockSpec((1, 2 * A, NE), lambda i, n: (i, 0, 0))
    cut = pl.BlockSpec((1, NX, 2 * A, Q), lambda i, n: (i, 0, 0, 0))
    return pl.pallas_call(
        pattern_kernel,
        grid_spec=pltpu.PrefetchScalarGridSpec(
            num_scalar_prefetch=1,
            grid=(steps,),
            in_specs=[
                pl.BlockSpec((NX, 2, 1, 2 * R, NE), at),
                pl.BlockSpec((NX, 2, 1, 2 * R, NE), at),
                pl.BlockSpec((NX, 2, 1, 2 * R, 2 * A), at),
            ],
            out_specs=[wide] * NX + [cut] * NY,
            scratch_shapes=[pltpu.VMEM((NX, 2 * A, NE), BF16)],
        ),
        out_shape=[jax.ShapeDtypeStruct((steps, 2 * A, NE), BF16)] * NX
        + [jax.ShapeDtypeStruct((steps, NX, 2 * A, Q), BF16)] * NY,
        compiler_params=params("arbitrary"),
        name="pattern",
    )(me, halves(keep), halves(recv), halves(fac))


def second_kernel(me, *refs):
    wide, cut = refs[:NX], refs[NX : NX + NY]
    by_y, by_x = refs[-NY - NX : -NX], refs[-NX:]
    for z in range(NZ // 2 // CHUNKS):
        for k in range(NY):
            at = pl.multiple_of(lax.rem(me[3] + k, NY) * Q, Q)
            by_y[k][z] = sum(r[z, :, pl.ds(at, Q)].astype(F32) for r in wide).astype(BF16)
        for k in range(NX):
            x = lax.rem(me[0] + k, NX)
            by_x[k][z] = sum(r[z, x].astype(F32) for r in cut).astype(BF16)


def second(me, wide, cut, chunk, earlier):
    rows = NZ // 2 // CHUNKS
    pieces = NY + NX
    out = jax.ShapeDtypeStruct((NZ // 2, 2 * A, Q), BF16)
    return pl.pallas_call(
        second_kernel,
        grid_spec=pltpu.PrefetchScalarGridSpec(
            num_scalar_prefetch=1,
            grid=(1,),
            in_specs=[pl.BlockSpec((rows, 2 * A, NE), lambda i, n: (0, 0, 0))] * NX
            + [pl.BlockSpec((rows, NX, 2 * A, Q), lambda i, n: (0, 0, 0, 0))] * NY
            + [pl.BlockSpec(memory_space=pl.ANY)] * len(earlier),
            out_specs=[pl.BlockSpec((rows, 2 * A, Q), lambda i, n: (chunk, 0, 0))] * pieces,
        ),
        out_shape=[out] * pieces,
        input_output_aliases={1 + pieces + i: i for i in range(len(earlier))},
        compiler_params=params("arbitrary"),
        name="second",
    )(me, *wide, *cut, *earlier)


def third_kernel(*refs):
    out = refs[-1]
    h = NZ // 2
    out[:h] = sum(r[...].astype(F32) for r in refs[:NY]).astype(BF16)
    out[h:] = sum(r[...].astype(F32) for r in refs[NY:-1]).astype(BF16)


def third(parts):
    return pl.pallas_call(
        third_kernel,
        out_shape=jax.ShapeDtypeStruct((NZ, 2 * A, Q), BF16),
        compiler_params=params(mb=4),
        name="third",
    )(*parts)


def last_kernel(parts, intensity, top):
    total = jnp.sum(parts[...].astype(F32), axis=0)
    value = total[:A] * total[:A] + total[A:] * total[A:]
    intensity[...] = value
    top[...] = jnp.broadcast_to(jnp.max(value, axis=0, keepdims=True)[None], top.shape)


def last(parts):
    return pl.pallas_call(
        last_kernel,
        out_shape=[
            jax.ShapeDtypeStruct((A, Q), F32),
            jax.ShapeDtypeStruct((NX * NZ * NC, 1, Q), F32),
        ],
        compiler_params=params(mb=4),
        name="last",
    )(parts)


def exchange(first, second, axes):
    firsts, seconds = [first[0]] + [None] * (NX - 1), [second[0]] + [None] * (NY - 1)
    for k in ORDER:
        firsts[k] = shift(first[k], axes[0], k)
        seconds[k] = shift(second[k], axes[1], k)
    return firsts, seconds


def body(currents, leaf_basis, leaf_box, box_count, merge_factor, angle_factor):
    me = jnp.stack([lax.axis_index(a).astype(jnp.int32) for a in ("x", "z", "c", "y")])
    own = turn(me, angle_factor)
    own = own.reshape(NX * NZ, NC * R, 2 * A)
    spread = lax.all_to_all(own, ("x", "z"), 0, 0, tiled=True)
    box = leaf_box.reshape(1, S_DEV)
    coefs = merge_factor.swapaxes(1, 2)
    keep, send = source(box_count, me, box, leaf_basis, currents, coefs)
    fac = spread.reshape(NX, NZ, NC * R, 2 * A)
    recv = shift(send, "c", 1)
    sent = []
    for chunk in range(CHUNKS):
        pieces = pattern(me, keep, recv, fac, chunk)
        sent.append(exchange(pieces[:NX], pieces[NX:], ("x", "y")))
    pieces = []
    for chunk in range(CHUNKS):
        pieces = second(me, *sent[chunk], chunk, pieces)
    firsts, seconds = exchange(pieces[:NY], pieces[NY:], ("y", "x"))
    parts = lax.all_to_all(third(firsts + seconds), "z", 0, 0, tiled=True)
    intensity, tops = last(parts)
    tops = lax.all_to_all(tops, ("x", "z", "c"), 0, 0, tiled=True)
    peak = jnp.max(tops, axis=(0, 1))
    return intensity / (peak[None, :] + 1.0), peak


def solution(mesh):
    split = Mesh(mesh.devices.reshape(NX, NZ, NC, NY), ("x", "z", "c", "y"))
    src, every = ("x", "z", "c"), ("x", "z", "c", "y")
    in_specs = (
        P(every, None),
        P(None, None, every),
        P(every),
        P(every),
        P(None, None, every),
        P(src, None, None, None),
    )
    out_specs = (P(src, "y"), P("y"))
    return jax.shard_map(body, mesh=split, in_specs=in_specs, out_specs=out_specs, check_vma=False)
```

```python
import jax
import jax.numpy as jnp
from jax import lax
from jax.experimental import pallas as pl
from jax.experimental.pallas import tpu as pltpu
from jax.sharding import Mesh
from jax.sharding import PartitionSpec as P


F32, BF16 = jnp.float32, jnp.bfloat16
NX, NZ, NC, NY = 4, 8, 2, 4
R, LEAF, S_DEV, NE, A = 40, 8, 2048, 512, 64
Q = NE // NY
LEAF_STEPS = 2
CHUNKS = 2
NEAR, FAR = (1, 3, 2), (2, 1, 3)


def other_core(v):
    return lax.ppermute(v, "c", [(0, 1), (1, 0)])


def shift(v, x_core, k):
    pairs = []
    for x in range(NX):
        for c in range(NC):
            for y in range(NY):
                to = ((x + k) % NX, y) if c == x_core else (x, (y + k) % NY)
                pairs.append(((x * NC + c) * NY + y, (to[0] * NC + c) * NY + to[1]))
    return lax.ppermute(v, ("x", "c", "y"), pairs)


def in_hbm(v):
    return pltpu.with_memory_space_constraint(v, pltpu.HBM)


def params(*sem, mb=16):
    return pltpu.CompilerParams(dimension_semantics=sem, vmem_limit_bytes=mb * 2**20)


def source_kernel(count, box, basis, x_re, x_im, m, keep, send, op, stacked):
    step = pl.program_id(0)
    half = LEAF * R

    @pl.when(step == 0)
    def _():
        boxes = box[...]
        for part in range(2):
            wide = basis[part].astype(F32)
            for pair in range(LEAF // 2):
                rows = []
                for b in (2 * pair, 2 * pair + 1):
                    scale = lax.rsqrt(jnp.full((1, S_DEV), count[b].astype(F32), F32))
                    rows.append(wide * jnp.where(boxes == b, scale, 0.0))
                at = part * half + pair * 2 * R
                op[at : at + 2 * R, :] = jnp.concatenate(rows, axis=0).astype(BF16)

    width = NE // LEAF_STEPS
    for k in range(LEAF_STEPS):

        @pl.when(step == k)
        def _(k=k):
            first = jnp.dot(op[...], x_re[...], preferred_element_type=F32)
            second = jnp.dot(op[...], x_im[...], preferred_element_type=F32)
            re = first[:half] - second[half:]
            im = second[:half] + first[half:]
            left, right = pl.ds(k * width, width), pl.ds(NE + k * width, width)
            stacked[:half, left] = re.astype(BF16)
            stacked[half:, left] = (-im).astype(BF16)
            stacked[:half, right] = im.astype(BF16)
            stacked[half:, right] = re.astype(BF16)

    @pl.when(step >= LEAF_STEPS)
    def _():
        rows = m[...].reshape(2 * half, NZ * NC * R).T
        out = jnp.dot(rows, stacked[...], preferred_element_type=F32)

        def write(own):
            for z in range(NZ):
                for c in range(NC):
                    g = (z * NC + c) * R
                    tile = [out[g : g + R, :NE], out[g : g + R, NE:]]
                    (keep if c == own else send)[0, z] = jnp.concatenate(tile, axis=0).astype(BF16)

        for own in range(NC):
            pl.when(lax.axis_index("c") == own)(lambda own=own: write(own))


def source(count, box, basis, currents, m):
    out = jax.ShapeDtypeStruct((NX, NZ, 2 * R, NE), BF16)
    width = NE // LEAF_STEPS

    def leaf_at(i):
        return jnp.minimum(i, LEAF_STEPS - 1)

    def merge_at(i):
        return jnp.maximum(i - LEAF_STEPS, 0)

    return pl.pallas_call(
        source_kernel,
        grid_spec=pltpu.PrefetchScalarGridSpec(
            num_scalar_prefetch=1,
            grid=(LEAF_STEPS + NX,),
            in_specs=[
                pl.BlockSpec((1, S_DEV), lambda i, *n: (0, 0)),
                pl.BlockSpec((2, R, S_DEV), lambda i, *n: (0, 0, 0)),
                pl.BlockSpec((S_DEV, width), lambda i, *n: (0, leaf_at(i))),
                pl.BlockSpec((S_DEV, width), lambda i, *n: (0, leaf_at(i) + LEAF_STEPS)),
                pl.BlockSpec((2, LEAF * R, NZ * NC * R), lambda i, *n: (0, 0, merge_at(i))),
            ],
            out_specs=[pl.BlockSpec((1, NZ, 2 * R, NE), lambda i, *n: (merge_at(i), 0, 0, 0))] * 2,
            scratch_shapes=[
                pltpu.VMEM((2 * LEAF * R, S_DEV), BF16),
                pltpu.VMEM((2 * LEAF * R, 2 * NE), BF16),
            ],
        ),
        out_shape=[out, out],
        compiler_params=params("arbitrary", mb=28),
        name="source",
    )(count, box, in_hbm(basis), in_hbm(currents), in_hbm(currents), in_hbm(m))


def turn_kernel(f, out):
    wide = f[:, 0].astype(F32)
    out[...] = jnp.concatenate([wide[:, 0], wide[:, 1]], axis=0).astype(BF16).T


def turn(factor):
    steps, columns = 2, factor.shape[3]
    width = columns // steps
    return pl.pallas_call(
        turn_kernel,
        grid=(steps,),
        in_specs=[pl.BlockSpec((A, 1, 2, width), lambda i: (0, lax.axis_index("y"), 0, i))],
        out_specs=pl.BlockSpec((width, 2 * A), lambda i: (i, 0)),
        out_shape=jax.ShapeDtypeStruct((columns, 2 * A), BF16),
        compiler_params=params("arbitrary"),
        name="turn",
    )(in_hbm(factor))


def pattern_kernel(keep, recv, fac, *refs):
    pieces, row = refs[:NX], refs[NX]
    core, x_own, y_own = (lax.axis_index(a) for a in ("c", "x", "y"))
    first = core == 0

    def product(x):
        both = fac[x, 0].astype(F32)
        turned = jnp.concatenate([-both[:, A:], both[:, :A]], axis=1)
        left = jnp.concatenate([both[:R], turned[:R], both[R:], turned[R:]], axis=0).astype(BF16)
        own, other = keep[x, 0], recv[x, 0]
        right = jnp.concatenate(
            [jnp.where(first, own, other), jnp.where(first, other, own)], axis=0
        )
        return jnp.dot(left.T, right, preferred_element_type=F32).astype(BF16)

    @pl.when(first)
    def _():
        for k in range(NX):
            piece = product(lax.rem(x_own + k, NX))
            for y in range(NY):
                pieces[k][0, y] = piece[:, y * Q : (y + 1) * Q]

    @pl.when(core == 1)
    def _():
        for x in range(NX):
            row[x] = product(x)
        for k in range(NY):
            at = pl.multiple_of(lax.rem(y_own + k, NY) * Q, Q)
            pieces[k][0] = row[:, :, pl.ds(at, Q)]


def pattern(keep, recv, fac, chunk):
    steps = NZ // CHUNKS

    def at(i):
        return (0, chunk * steps + i, 0, 0)

    return pl.pallas_call(
        pattern_kernel,
        grid=(steps,),
        in_specs=[
            pl.BlockSpec((NX, 1, 2 * R, NE), at),
            pl.BlockSpec((NX, 1, 2 * R, NE), at),
            pl.BlockSpec((NX, 1, 2 * R, 2 * A), at),
        ],
        out_specs=[pl.BlockSpec((1, NX, 2 * A, Q), lambda i: (i, 0, 0, 0))] * NX,
        out_shape=[jax.ShapeDtypeStruct((steps, NX, 2 * A, Q), BF16)] * NX,
        scratch_shapes=[pltpu.VMEM((NX, 2 * A, NE), BF16)],
        compiler_params=params("arbitrary"),
        name="pattern",
    )(keep, recv, fac)


def second_kernel(*refs):
    parts, pieces = refs[:NX], refs[-NX:]
    own = jnp.where(lax.axis_index("c") == 0, lax.axis_index("y"), lax.axis_index("x"))
    for k in range(NX):
        at = lax.rem(own + k, NX)
        for z in range(NZ // CHUNKS):
            pieces[k][z] = sum(r[z, at].astype(F32) for r in parts).astype(BF16)


def second(parts, chunk, earlier):
    rows = NZ // CHUNKS
    return pl.pallas_call(
        second_kernel,
        grid=(1,),
        in_specs=[pl.BlockSpec((rows, NX, 2 * A, Q), lambda i: (0, 0, 0, 0))] * NX
        + [pl.BlockSpec(memory_space=pl.ANY)] * len(earlier),
        out_specs=[pl.BlockSpec((rows, 2 * A, Q), lambda i: (chunk, 0, 0))] * NX,
        out_shape=[jax.ShapeDtypeStruct((NZ, 2 * A, Q), BF16)] * NX,
        input_output_aliases={NX + i: i for i in range(len(earlier))},
        compiler_params=params("arbitrary"),
        name="second",
    )(*parts, *earlier)


def third_kernel(*refs):
    refs[-1][...] = sum(r[...].astype(F32) for r in refs[:-1]).astype(BF16)


def third(parts):
    return pl.pallas_call(
        third_kernel,
        out_shape=jax.ShapeDtypeStruct((NZ, 2 * A, Q), BF16),
        compiler_params=params(mb=4),
        name="third",
    )(*parts)


def last_kernel(parts, intensity, top):
    total = jnp.sum(parts[...].astype(F32), axis=0)
    value = total[:A] * total[:A] + total[A:] * total[A:]
    intensity[...] = value
    top[...] = jnp.broadcast_to(jnp.max(value, axis=0, keepdims=True)[None], top.shape)


def last(parts):
    return pl.pallas_call(
        last_kernel,
        out_shape=[
            jax.ShapeDtypeStruct((A, Q), F32),
            jax.ShapeDtypeStruct((NX * NZ * NC, 1, Q), F32),
        ],
        compiler_params=params(mb=4),
        name="last",
    )(parts)


def exchange(pieces, x_core, order):
    parts = [pieces[0]] + [None] * (NX - 1)
    for k in order:
        parts[k] = shift(pieces[k], x_core, k)
    return parts


def body(currents, leaf_basis, leaf_box, box_count, merge_factor, angle_factor):
    own = turn(angle_factor)
    own = own.reshape(NX * NZ, NC * R, 2 * A)
    spread = lax.all_to_all(own, ("x", "z"), 0, 0, tiled=True)
    box = leaf_box.reshape(1, S_DEV)
    coefs = merge_factor.swapaxes(1, 2)
    keep, send = source(box_count, box, leaf_basis, currents, coefs)
    fac = spread.reshape(NX, NZ, NC * R, 2 * A)
    recv = other_core(send)
    sent = []
    for chunk in range(CHUNKS):
        pieces = pattern(keep, recv, fac, chunk)
        sent.append(exchange(pieces, 0, NEAR))
    pieces = []
    for chunk in range(CHUNKS):
        pieces = second(sent[chunk], chunk, pieces)
    parts = third(exchange(pieces, 1, FAR))
    parts = lax.all_to_all(parts, "z", 0, 0, tiled=True)
    intensity, tops = last(parts)
    tops = lax.all_to_all(tops, ("x", "z", "c"), 0, 0, tiled=True)
    peak = jnp.max(tops, axis=(0, 1))
    return intensity / (peak[None, :] + 1.0), peak


def solution(mesh):
    split = Mesh(mesh.devices.reshape(NX, NZ, NC, NY), ("x", "z", "c", "y"))
    src, every = ("x", "z", "c"), ("x", "z", "c", "y")
    in_specs = (
        P(every, None),
        P(None, None, every),
        P(every),
        P(every),
        P(None, None, every),
        P(src, None, None, None),
    )
    out_specs = (P(src, "y"), P("y"))
    return jax.shard_map(body, mesh=split, in_specs=in_specs, out_specs=out_specs, check_vma=False)
```

```python
import jax
import jax.numpy as jnp
from jax import lax
from jax.experimental import pallas as pl
from jax.experimental.pallas import tpu as pltpu
from jax.sharding import Mesh
from jax.sharding import PartitionSpec as P


F32, BF16 = jnp.float32, jnp.bfloat16
NX, NZ, NC, NY = 4, 8, 2, 4
R, LEAF, S_DEV, NE, A = 40, 8, 2048, 512, 64
Q = NE // NY
LEAF_STEPS = 2
CHUNKS = 2
FAR = (2, 1, 3)
PLACE = {0: 0, 1: 1, 3: 2}


def other_core(v):
    return lax.ppermute(v, "c", [(0, 1), (1, 0)])


def shift(v, x_core, k):
    pairs = []
    for x in range(NX):
        for c in range(NC):
            for y in range(NY):
                to = ((x + k) % NX, y) if c == x_core else (x, (y + k) % NY)
                pairs.append(((x * NC + c) * NY + y, (to[0] * NC + c) * NY + to[1]))
    return lax.ppermute(v, ("x", "c", "y"), pairs)


def in_hbm(v):
    return pltpu.with_memory_space_constraint(v, pltpu.HBM)


def params(*sem, mb=16):
    return pltpu.CompilerParams(dimension_semantics=sem, vmem_limit_bytes=mb * 2**20)


def source_kernel(count, box, basis, x_re, x_im, m, keep, send, op, stacked):
    step = pl.program_id(0)
    half = LEAF * R

    @pl.when(step == 0)
    def _():
        boxes = box[...]
        for part in range(2):
            wide = basis[part].astype(F32)
            for pair in range(LEAF // 2):
                rows = []
                for b in (2 * pair, 2 * pair + 1):
                    scale = lax.rsqrt(jnp.full((1, S_DEV), count[b].astype(F32), F32))
                    rows.append(wide * jnp.where(boxes == b, scale, 0.0))
                at = part * half + pair * 2 * R
                op[at : at + 2 * R, :] = jnp.concatenate(rows, axis=0).astype(BF16)

    width = NE // LEAF_STEPS
    for k in range(LEAF_STEPS):

        @pl.when(step == k)
        def _(k=k):
            first = jnp.dot(op[...], x_re[...], preferred_element_type=F32)
            second = jnp.dot(op[...], x_im[...], preferred_element_type=F32)
            re = first[:half] - second[half:]
            im = second[:half] + first[half:]
            left, right = pl.ds(k * width, width), pl.ds(NE + k * width, width)
            stacked[:half, left] = re.astype(BF16)
            stacked[half:, left] = (-im).astype(BF16)
            stacked[:half, right] = im.astype(BF16)
            stacked[half:, right] = re.astype(BF16)

    @pl.when(step >= LEAF_STEPS)
    def _():
        rows = m[...].reshape(2 * half, NZ * NC * R).T
        out = jnp.dot(rows, stacked[...], preferred_element_type=F32)

        def write(own):
            for z in range(NZ):
                for c in range(NC):
                    g = (z * NC + c) * R
                    tile = [out[g : g + R, :NE], out[g : g + R, NE:]]
                    (keep if c == own else send)[0, z] = jnp.concatenate(tile, axis=0).astype(BF16)

        for own in range(NC):
            pl.when(lax.axis_index("c") == own)(lambda own=own: write(own))


def source(count, box, basis, currents, m):
    out = jax.ShapeDtypeStruct((NX, NZ, 2 * R, NE), BF16)
    width = NE // LEAF_STEPS

    def leaf_at(i):
        return jnp.minimum(i, LEAF_STEPS - 1)

    def merge_at(i):
        return jnp.maximum(i - LEAF_STEPS, 0)

    return pl.pallas_call(
        source_kernel,
        grid_spec=pltpu.PrefetchScalarGridSpec(
            num_scalar_prefetch=1,
            grid=(LEAF_STEPS + NX,),
            in_specs=[
                pl.BlockSpec((1, S_DEV), lambda i, *n: (0, 0)),
                pl.BlockSpec((2, R, S_DEV), lambda i, *n: (0, 0, 0)),
                pl.BlockSpec((S_DEV, width), lambda i, *n: (0, leaf_at(i))),
                pl.BlockSpec((S_DEV, width), lambda i, *n: (0, leaf_at(i) + LEAF_STEPS)),
                pl.BlockSpec((2, LEAF * R, NZ * NC * R), lambda i, *n: (0, 0, merge_at(i))),
            ],
            out_specs=[pl.BlockSpec((1, NZ, 2 * R, NE), lambda i, *n: (merge_at(i), 0, 0, 0))] * 2,
            scratch_shapes=[
                pltpu.VMEM((2 * LEAF * R, S_DEV), BF16),
                pltpu.VMEM((2 * LEAF * R, 2 * NE), BF16),
            ],
        ),
        out_shape=[out, out],
        compiler_params=params("arbitrary", mb=28),
        name="source",
    )(count, box, in_hbm(basis), in_hbm(currents), in_hbm(currents), in_hbm(m))


def turn_kernel(f, out):
    wide = f[:, 0].astype(F32)
    out[...] = jnp.concatenate([wide[:, 0], wide[:, 1]], axis=0).astype(BF16).T


def turn(factor):
    steps, columns = 2, factor.shape[3]
    width = columns // steps
    return pl.pallas_call(
        turn_kernel,
        grid=(steps,),
        in_specs=[pl.BlockSpec((A, 1, 2, width), lambda i: (0, lax.axis_index("y"), 0, i))],
        out_specs=pl.BlockSpec((width, 2 * A), lambda i: (i, 0)),
        out_shape=jax.ShapeDtypeStruct((columns, 2 * A), BF16),
        compiler_params=params("arbitrary"),
        name="turn",
    )(in_hbm(factor))


def pattern_kernel(keep, recv, fac, *refs):
    pieces, halves, row = refs[:3], refs[3:5], refs[5]
    core, x_own, y_own = (lax.axis_index(a) for a in ("c", "x", "y"))
    first = core == 0

    def product(x):
        both = fac[x, 0].astype(F32)
        turned = jnp.concatenate([-both[:, A:], both[:, :A]], axis=1)
        left = jnp.concatenate([both[:R], turned[:R], both[R:], turned[R:]], axis=0).astype(BF16)
        own, other = keep[x, 0], recv[x, 0]
        right = jnp.concatenate(
            [jnp.where(first, own, other), jnp.where(first, other, own)], axis=0
        )
        return jnp.dot(left.T, right, preferred_element_type=F32).astype(BF16)

    @pl.when(core == 1)
    def _():
        for k in range(NX):
            piece = product(lax.rem(x_own + k, NX))
            for y in range(NY):
                to = halves[y // 2].at[0, y % 2] if k == 2 else pieces[PLACE[k]].at[0, y]
                to[...] = piece[:, y * Q : (y + 1) * Q]

    @pl.when(core == 0)
    def _():
        for x in range(NX):
            row[x] = product(x)
        for k in range(NY):
            at = pl.multiple_of(lax.rem(y_own + k, NY) * Q, Q)
            if k == 2:
                for half in range(2):
                    halves[half][0] = row[2 * half : 2 * half + 2, :, pl.ds(at, Q)]
            else:
                pieces[PLACE[k]][0] = row[:, :, pl.ds(at, Q)]


def pattern(keep, recv, fac, chunk):
    steps = NZ // CHUNKS

    def at(i):
        return (0, chunk * steps + i, 0, 0)

    return pl.pallas_call(
        pattern_kernel,
        grid=(steps,),
        in_specs=[
            pl.BlockSpec((NX, 1, 2 * R, NE), at),
            pl.BlockSpec((NX, 1, 2 * R, NE), at),
            pl.BlockSpec((NX, 1, 2 * R, 2 * A), at),
        ],
        out_specs=[pl.BlockSpec((1, NX, 2 * A, Q), lambda i: (i, 0, 0, 0))] * 3
        + [pl.BlockSpec((1, NX // 2, 2 * A, Q), lambda i: (i, 0, 0, 0))] * 2,
        out_shape=[jax.ShapeDtypeStruct((steps, NX, 2 * A, Q), BF16)] * 3
        + [jax.ShapeDtypeStruct((steps, NX // 2, 2 * A, Q), BF16)] * 2,
        scratch_shapes=[pltpu.VMEM((NX, 2 * A, NE), BF16)],
        compiler_params=params("arbitrary"),
        name="pattern",
    )(keep, recv, fac)


def forward_kernel(ahead, behind, from_behind, from_ahead, to_ahead, to_behind):
    h = NX // 2
    for z in range(NZ // CHUNKS):
        to_ahead[z, :h] = (ahead[z, :h].astype(F32) + from_behind[z].astype(F32)).astype(BF16)
        to_ahead[z, h:] = ahead[z, h:]
        to_behind[z, :h] = behind[z, :h]
        to_behind[z, h:] = (behind[z, h:].astype(F32) + from_ahead[z].astype(F32)).astype(BF16)


def forward(*pieces):
    return pl.pallas_call(
        forward_kernel,
        out_shape=[jax.ShapeDtypeStruct(pieces[0].shape, BF16)] * 2,
        compiler_params=params(mb=10),
        name="forward",
    )(*pieces)


def second_kernel(*refs):
    parts, pieces = refs[:3], refs[-NX:]
    own = jnp.where(lax.axis_index("c") == 1, lax.axis_index("y"), lax.axis_index("x"))
    for k in range(NX):
        at = lax.rem(own + k, NX)
        for z in range(NZ // CHUNKS):
            pieces[k][z] = sum(r[z, at].astype(F32) for r in parts).astype(BF16)


def second(parts, chunk, earlier):
    rows = NZ // CHUNKS
    return pl.pallas_call(
        second_kernel,
        grid=(1,),
        in_specs=[pl.BlockSpec((rows, NX, 2 * A, Q), lambda i: (0, 0, 0, 0))] * 3
        + [pl.BlockSpec(memory_space=pl.ANY)] * len(earlier),
        out_specs=[pl.BlockSpec((rows, 2 * A, Q), lambda i: (chunk, 0, 0))] * NX,
        out_shape=[jax.ShapeDtypeStruct((NZ, 2 * A, Q), BF16)] * NX,
        input_output_aliases={3 + i: i for i in range(len(earlier))},
        compiler_params=params("arbitrary"),
        name="second",
    )(*parts, *earlier)


def third_kernel(*refs):
    refs[-1][...] = sum(r[...].astype(F32) for r in refs[:-1]).astype(BF16)


def third(parts):
    return pl.pallas_call(
        third_kernel,
        out_shape=jax.ShapeDtypeStruct((NZ, 2 * A, Q), BF16),
        compiler_params=params(mb=4),
        name="third",
    )(*parts)


def last_kernel(parts, intensity, top):
    total = jnp.sum(parts[...].astype(F32), axis=0)
    value = total[:A] * total[:A] + total[A:] * total[A:]
    intensity[...] = value
    top[...] = jnp.broadcast_to(jnp.max(value, axis=0, keepdims=True)[None], top.shape)


def last(parts):
    return pl.pallas_call(
        last_kernel,
        out_shape=[
            jax.ShapeDtypeStruct((A, Q), F32),
            jax.ShapeDtypeStruct((NX * NZ * NC, 1, Q), F32),
        ],
        compiler_params=params(mb=4),
        name="last",
    )(parts)


def exchange(pieces, x_core, order):
    parts = [pieces[0]] + [None] * (NX - 1)
    for k in order:
        parts[k] = shift(pieces[k], x_core, k)
    return parts


def both_ways(ahead, behind):
    ahead = shift(ahead, 1, 1)
    behind = shift(behind, 1, NX - 1)
    return ahead, behind


def body(currents, leaf_basis, leaf_box, box_count, merge_factor, angle_factor):
    own = turn(angle_factor)
    own = own.reshape(NX * NZ, NC * R, 2 * A)
    spread = lax.all_to_all(own, ("x", "z"), 0, 0, tiled=True)
    box = leaf_box.reshape(1, S_DEV)
    coefs = merge_factor.swapaxes(1, 2)
    keep, send = source(box_count, box, leaf_basis, currents, coefs)
    fac = spread.reshape(NX, NZ, NC * R, 2 * A)
    recv = other_core(send)
    made, sums = [], []
    for chunk in range(CHUNKS):
        pieces = pattern(keep, recv, fac, chunk)
        made.append((pieces, both_ways(*pieces[3:])))
    for pieces, halves in made:
        ahead, behind = forward(*pieces[1:3], *halves)
        sums.append([pieces[0], *both_ways(ahead, behind)])
    pieces = []
    for chunk in range(CHUNKS):
        pieces = second(sums[chunk], chunk, pieces)
    parts = third(exchange(pieces, 0, FAR))
    parts = lax.all_to_all(parts, "z", 0, 0, tiled=True)
    intensity, tops = last(parts)
    tops = lax.all_to_all(tops, ("x", "z", "c"), 0, 0, tiled=True)
    peak = jnp.max(tops, axis=(0, 1))
    return intensity / (peak[None, :] + 1.0), peak


def solution(mesh):
    split = Mesh(mesh.devices.reshape(NX, NZ, NC, NY), ("x", "z", "c", "y"))
    src, every = ("x", "z", "c"), ("x", "z", "c", "y")
    in_specs = (
        P(every, None),
        P(None, None, every),
        P(every),
        P(every),
        P(None, None, every),
        P(src, None, None, None),
    )
    out_specs = (P(src, "y"), P("y"))
    return jax.shard_map(body, mesh=split, in_specs=in_specs, out_specs=out_specs, check_vma=False)
```

```python
import jax
import jax.numpy as jnp
from jax import lax
from jax.experimental import pallas as pl
from jax.experimental.pallas import tpu as pltpu
from jax.sharding import Mesh
from jax.sharding import PartitionSpec as P


F32, BF16 = jnp.float32, jnp.bfloat16
NX, NZ, NC, NY = 4, 8, 2, 4
R, LEAF, S_DEV, NE, A = 40, 8, 2048, 512, 64
Q = NE // NY
LEAF_STEPS = 2
CHUNKS = 2
ZB = 2
FAR = (2, 1, 3)
PLACE = {0: 0, 1: 1, 3: 2}


def other_core(v):
    return lax.ppermute(v, "c", [(0, 1), (1, 0)])


def shift(v, x_core, k):
    pairs = []
    for x in range(NX):
        for c in range(NC):
            for y in range(NY):
                to = ((x + k) % NX, y) if c == x_core else (x, (y + k) % NY)
                pairs.append(((x * NC + c) * NY + y, (to[0] * NC + c) * NY + to[1]))
    return lax.ppermute(v, ("x", "c", "y"), pairs)


def in_hbm(v):
    return pltpu.with_memory_space_constraint(v, pltpu.HBM)


def params(*sem, mb=16):
    return pltpu.CompilerParams(dimension_semantics=sem, vmem_limit_bytes=mb * 2**20)


def source_kernel(count, box, basis, x_re, x_im, m, keep, send, op, stacked):
    step = pl.program_id(0)
    half = LEAF * R

    @pl.when(step == 0)
    def _():
        boxes = box[...]
        for part in range(2):
            wide = basis[part].astype(F32)
            for pair in range(LEAF // 2):
                rows = []
                for b in (2 * pair, 2 * pair + 1):
                    scale = lax.rsqrt(jnp.full((1, S_DEV), count[b].astype(F32), F32))
                    rows.append(wide * jnp.where(boxes == b, scale, 0.0))
                at = part * half + pair * 2 * R
                op[at : at + 2 * R, :] = jnp.concatenate(rows, axis=0).astype(BF16)

    width = NE // LEAF_STEPS
    for k in range(LEAF_STEPS):

        @pl.when(step == k)
        def _(k=k):
            first = jnp.dot(op[...], x_re[...], preferred_element_type=F32)
            second = jnp.dot(op[...], x_im[...], preferred_element_type=F32)
            re = first[:half] - second[half:]
            im = second[:half] + first[half:]
            left, right = pl.ds(k * width, width), pl.ds(NE + k * width, width)
            stacked[:half, left] = re.astype(BF16)
            stacked[half:, left] = (-im).astype(BF16)
            stacked[:half, right] = im.astype(BF16)
            stacked[half:, right] = re.astype(BF16)

    @pl.when(step >= LEAF_STEPS)
    def _():
        rows = m[...].reshape(2 * half, NZ * NC * R).T
        out = jnp.dot(rows, stacked[...], preferred_element_type=F32)

        def write(own):
            for z in range(NZ):
                for c in range(NC):
                    g = (z * NC + c) * R
                    tile = [out[g : g + R, :NE], out[g : g + R, NE:]]
                    (keep if c == own else send)[0, z] = jnp.concatenate(tile, axis=0).astype(BF16)

        for own in range(NC):
            pl.when(lax.axis_index("c") == own)(lambda own=own: write(own))


def source(count, box, basis, currents, m):
    out = jax.ShapeDtypeStruct((NX, NZ, 2 * R, NE), BF16)
    width = NE // LEAF_STEPS

    def leaf_at(i):
        return jnp.minimum(i, LEAF_STEPS - 1)

    def merge_at(i):
        return jnp.maximum(i - LEAF_STEPS, 0)

    return pl.pallas_call(
        source_kernel,
        grid_spec=pltpu.PrefetchScalarGridSpec(
            num_scalar_prefetch=1,
            grid=(LEAF_STEPS + NX,),
            in_specs=[
                pl.BlockSpec((1, S_DEV), lambda i, *n: (0, 0)),
                pl.BlockSpec((2, R, S_DEV), lambda i, *n: (0, 0, 0)),
                pl.BlockSpec((S_DEV, width), lambda i, *n: (0, leaf_at(i))),
                pl.BlockSpec((S_DEV, width), lambda i, *n: (0, leaf_at(i) + LEAF_STEPS)),
                pl.BlockSpec((2, LEAF * R, NZ * NC * R), lambda i, *n: (0, 0, merge_at(i))),
            ],
            out_specs=[pl.BlockSpec((1, NZ, 2 * R, NE), lambda i, *n: (merge_at(i), 0, 0, 0))] * 2,
            scratch_shapes=[
                pltpu.VMEM((2 * LEAF * R, S_DEV), BF16),
                pltpu.VMEM((2 * LEAF * R, 2 * NE), BF16),
            ],
        ),
        out_shape=[out, out],
        compiler_params=params("arbitrary", mb=28),
        name="source",
    )(count, box, in_hbm(basis), in_hbm(currents), in_hbm(currents), in_hbm(m))


def turn_kernel(f, out):
    wide = f[:, 0].astype(F32)
    turned = jnp.concatenate([wide[:, 0], wide[:, 1]], axis=0).astype(BF16).T
    rows = NC * R
    for x in range(NX // 2):
        for z in range(NZ):
            at = (x * NZ + z) * rows
            out[z, x] = turned[at : at + rows]


def turn(factor):
    steps, columns = 2, factor.shape[3]
    width = columns // steps
    return pl.pallas_call(
        turn_kernel,
        grid=(steps,),
        in_specs=[pl.BlockSpec((A, 1, 2, width), lambda i: (0, lax.axis_index("y"), 0, i))],
        out_specs=pl.BlockSpec((NZ, NX // steps, NC * R, 2 * A), lambda i: (0, i, 0, 0)),
        out_shape=jax.ShapeDtypeStruct((NZ, NX, NC * R, 2 * A), BF16),
        compiler_params=params("arbitrary"),
        name="turn",
    )(in_hbm(factor))


def pattern_kernel(keep, recv, fac, *refs):
    pieces, halves, row = refs[:3], refs[3:5], refs[5]
    core, x_own, y_own = (lax.axis_index(a) for a in ("c", "x", "y"))
    first = core == 0

    def product(x, z):
        both = fac[z, x].astype(F32)
        turned = jnp.concatenate([-both[:, A:], both[:, :A]], axis=1)
        left = jnp.concatenate([both[:R], turned[:R], both[R:], turned[R:]], axis=0).astype(BF16)
        own, other = keep[x, z], recv[x, z]
        right = jnp.concatenate(
            [jnp.where(first, own, other), jnp.where(first, other, own)], axis=0
        )
        return jnp.dot(left.T, right, preferred_element_type=F32).astype(BF16)

    @pl.when(core == 1)
    def _():
        for z in range(ZB):
            for k in range(NX):
                piece = product(lax.rem(x_own + k, NX), z)
                for y in range(NY):
                    to = halves[y // 2].at[z, y % 2] if k == 2 else pieces[PLACE[k]].at[z, y]
                    to[...] = piece[:, y * Q : (y + 1) * Q]

    @pl.when(core == 0)
    def _():
        for z in range(ZB):
            for x in range(NX):
                row[z, x] = product(x, z)
        for k in range(NY):
            at = pl.multiple_of(lax.rem(y_own + k, NY) * Q, Q)
            if k == 2:
                for half in range(2):
                    halves[half][...] = row[:, 2 * half : 2 * half + 2, :, pl.ds(at, Q)]
            else:
                pieces[PLACE[k]][...] = row[:, :, :, pl.ds(at, Q)]


def pattern(keep, recv, fac, chunk):
    rows = NZ // CHUNKS
    steps = rows // ZB

    def at(i):
        return (0, chunk * steps + i, 0, 0)

    return pl.pallas_call(
        pattern_kernel,
        grid=(steps,),
        in_specs=[
            pl.BlockSpec((NX, ZB, 2 * R, NE), at),
            pl.BlockSpec((NX, ZB, 2 * R, NE), at),
            pl.BlockSpec((ZB, NX, 2 * R, 2 * A), lambda i: (chunk * steps + i, 0, 0, 0)),
        ],
        out_specs=[pl.BlockSpec((ZB, NX, 2 * A, Q), lambda i: (i, 0, 0, 0))] * 3
        + [pl.BlockSpec((ZB, NX // 2, 2 * A, Q), lambda i: (i, 0, 0, 0))] * 2,
        out_shape=[jax.ShapeDtypeStruct((rows, NX, 2 * A, Q), BF16)] * 3
        + [jax.ShapeDtypeStruct((rows, NX // 2, 2 * A, Q), BF16)] * 2,
        scratch_shapes=[pltpu.VMEM((ZB, NX, 2 * A, NE), BF16)],
        compiler_params=params("arbitrary"),
        name="pattern",
    )(keep, recv, fac)


def forward_kernel(ahead, behind, from_behind, from_ahead, to_ahead, to_behind):
    h = NX // 2
    for z in range(NZ // CHUNKS):
        to_ahead[z, :h] = (ahead[z, :h].astype(F32) + from_behind[z].astype(F32)).astype(BF16)
        to_ahead[z, h:] = ahead[z, h:]
        to_behind[z, :h] = behind[z, :h]
        to_behind[z, h:] = (behind[z, h:].astype(F32) + from_ahead[z].astype(F32)).astype(BF16)


def forward(*pieces):
    return pl.pallas_call(
        forward_kernel,
        out_shape=[jax.ShapeDtypeStruct(pieces[0].shape, BF16)] * 2,
        compiler_params=params(mb=10),
        name="forward",
    )(*pieces)


def second_kernel(*refs):
    parts, pieces = refs[:3], refs[-NX:]
    own = jnp.where(lax.axis_index("c") == 1, lax.axis_index("y"), lax.axis_index("x"))
    for k in range(NX):
        at = lax.rem(own + k, NX)
        for z in range(NZ // CHUNKS):
            pieces[k][z] = sum(r[z, at].astype(F32) for r in parts).astype(BF16)


def second(parts, chunk, earlier):
    rows = NZ // CHUNKS
    return pl.pallas_call(
        second_kernel,
        grid=(1,),
        in_specs=[pl.BlockSpec((rows, NX, 2 * A, Q), lambda i: (0, 0, 0, 0))] * 3
        + [pl.BlockSpec(memory_space=pl.ANY)] * len(earlier),
        out_specs=[pl.BlockSpec((rows, 2 * A, Q), lambda i: (chunk, 0, 0))] * NX,
        out_shape=[jax.ShapeDtypeStruct((NZ, 2 * A, Q), BF16)] * NX,
        input_output_aliases={3 + i: i for i in range(len(earlier))},
        compiler_params=params("arbitrary"),
        name="second",
    )(*parts, *earlier)


def third_kernel(*refs):
    refs[-1][...] = sum(r[...].astype(F32) for r in refs[:-1]).astype(BF16)


def third(parts):
    return pl.pallas_call(
        third_kernel,
        out_shape=jax.ShapeDtypeStruct((NZ, 2 * A, Q), BF16),
        compiler_params=params(mb=4),
        name="third",
    )(*parts)


def last_kernel(parts, intensity, top):
    total = jnp.sum(parts[...].astype(F32), axis=0)
    value = total[:A] * total[:A] + total[A:] * total[A:]
    intensity[...] = value
    top[...] = jnp.broadcast_to(jnp.max(value, axis=0, keepdims=True)[None], top.shape)


def last(parts):
    return pl.pallas_call(
        last_kernel,
        out_shape=[
            jax.ShapeDtypeStruct((A, Q), F32),
            jax.ShapeDtypeStruct((NX * NZ * NC, 1, Q), F32),
        ],
        compiler_params=params(mb=4),
        name="last",
    )(parts)


def exchange(pieces, x_core, order):
    parts = [pieces[0]] + [None] * (NX - 1)
    for k in order:
        parts[k] = shift(pieces[k], x_core, k)
    return parts


def both_ways(ahead, behind):
    ahead = shift(ahead, 1, 1)
    behind = shift(behind, 1, NX - 1)
    return ahead, behind


def body(currents, leaf_basis, leaf_box, box_count, merge_factor, angle_factor):
    own = turn(angle_factor)
    own = own.reshape(NX * NZ, NC * R, 2 * A)
    spread = lax.all_to_all(own, ("z", "x"), 0, 0, tiled=True)
    box = leaf_box.reshape(1, S_DEV)
    coefs = merge_factor.swapaxes(1, 2)
    keep, send = source(box_count, box, leaf_basis, currents, coefs)
    fac = spread.reshape(NZ, NX, NC * R, 2 * A)
    recv = other_core(send)
    made, sums = [], []
    for chunk in range(CHUNKS):
        pieces = pattern(keep, recv, fac, chunk)
        made.append((pieces, both_ways(*pieces[3:])))
    for pieces, halves in made:
        ahead, behind = forward(*pieces[1:3], *halves)
        sums.append([pieces[0], *both_ways(ahead, behind)])
    pieces = []
    for chunk in range(CHUNKS):
        pieces = second(sums[chunk], chunk, pieces)
    parts = third(exchange(pieces, 0, FAR))
    parts = lax.all_to_all(parts, "z", 0, 0, tiled=True)
    intensity, tops = last(parts)
    tops = lax.all_to_all(tops, ("x", "z", "c"), 0, 0, tiled=True)
    peak = jnp.max(tops, axis=(0, 1))
    return intensity / (peak[None, :] + 1.0), peak


def solution(mesh):
    split = Mesh(mesh.devices.reshape(NX, NZ, NC, NY), ("x", "z", "c", "y"))
    src, every = ("x", "z", "c"), ("x", "z", "c", "y")
    in_specs = (
        P(every, None),
        P(None, None, every),
        P(every),
        P(every),
        P(None, None, every),
        P(src, None, None, None),
    )
    out_specs = (P(src, "y"), P("y"))
    return jax.shard_map(body, mesh=split, in_specs=in_specs, out_specs=out_specs, check_vma=False)
```
